16 devices in a mesh: data: 2 (over y, z), tp: 8 (over x, core).
Axes of the slice: x: 4, y: 2, z: 1, core: 2. Of those that a mesh axis runs over, the one named last changes fastest.
The devices are a block of a 4x4x8 slice.
Arguments:
- x: bfloat16 [8192, 28672], P('data', 'tp'), parts along dimension 0
- w: bfloat16 [28672, 8192], P('tp')
- lengths: int32 [8], P('data'), parts along dimension 0
Outputs:
- output: bfloat16 [8192, 8192], P('data'), parts along dimension 0
There are 2 independent parts. The reference program is written for one: setup_inputs(seed, part) draws one part's arguments, and reference() takes and returns one part's arrays. A program takes and returns all parts, laid end to end along the dimension named above; an argument that names none is the same for every part.
All inputs are finite; a program needn't handle non-finite values.
Results may differ from the reference program's by a relative error of at most 0.001.
Values are sent between devices in bfloat16 or wider.
A program may use at most 768 MiB of HBM per device.

```python
import jax
import jax.numpy as jnp

D = 8192
FF = 28672
TOKENS = 4096
SEQS = 4
SEQ_LEN = TOKENS // SEQS


def draw_lengths(key_len):
    key_draw, key_perm = jax.random.split(key_len)
    lengths = jax.random.randint(key_draw, (SEQS,), 1, SEQ_LEN + 1, dtype=jnp.int32)
    slot_order = jax.random.permutation(key_perm, SEQS)
    lengths = lengths.at[slot_order[0]].set(SEQ_LEN)
    lengths = lengths.at[slot_order[1]].set(1)
    return lengths


def setup_inputs(seed: int = 0, part: int = 0) -> dict:
    key = jax.random.key(seed)
    key_x, key_w, key_len = jax.random.split(key, 3)
    tok_acts = jax.random.normal(jax.random.fold_in(key_x, part), (TOKENS, FF), jnp.float32)
    weight = jax.random.normal(key_w, (FF, D), jnp.float32) * (FF ** -0.5)
    lengths = draw_lengths(jax.random.fold_in(key_len, part))
    return {"x": tok_acts.astype(jnp.bfloat16), "w": weight.astype(jnp.bfloat16), "lengths": lengths}


def reference(x, w, lengths):
    seq_len = x.shape[0] // lengths.shape[0]
    valid = (jnp.arange(seq_len, dtype=jnp.int32)[None, :] < lengths[:, None]).reshape(-1)
    full_sum = jnp.dot(x, w, preferred_element_type=jnp.float32)
    return jnp.where(valid[:, None], full_sum, 0.0).astype(jnp.bfloat16)
```

```python
import functools

import jax
import jax.numpy as jnp
from jax import lax
from jax.experimental import pallas as pl
from jax.experimental.pallas import tpu as pltpu
from jax.sharding import PartitionSpec as P

MESH = pl.DeviceIdType.MESH
ROW_BLOCK = 16
BUCKET_STEP = 256
CHUNK_COLS = 512
OUT_TILE = 256
SLOTS = 3
DOT_ROWS = 256
BF16_MAX = float(jnp.finfo(jnp.bfloat16).max)


def spacing(high):
    size = jnp.abs(high)
    above = (size * (1 + 0.75 / 128)).astype(jnp.bfloat16).astype(jnp.float32)
    return jnp.clip(above - size, 2.0**-120, 2.0**120)


def encode(values):
    highs, digits = [], []
    for v in values:
        high = jnp.clip(v, -BF16_MAX, BF16_MAX).astype(jnp.bfloat16)
        full = high.astype(jnp.float32)
        rest = (v - full) / spacing(full)
        highs.append(high)
        digits.append(jnp.clip(jnp.floor(rest * 15 + 0.5), -7, 7))
    n = digits[0] + 15 * digits[1] + 112
    e = digits[2] + 15 * digits[3]
    word = jnp.where(n < 128, n + 128, -n) * jnp.exp2(e)
    return highs, word.astype(jnp.bfloat16)


def decode(highs, word):
    word = word.astype(jnp.float32)
    size = jnp.abs(word)
    e = jnp.floor(jnp.log2(size) + (0.002 - 7))
    m = jnp.floor(size * jnp.exp2(-e) + 0.5)
    n = jnp.where(word > 0, m - 240, m - 112)
    values = []
    for k, code in enumerate((n, e)):
        second = jnp.floor(code * (1 / 15) + 0.5)
        for high, digit in zip(highs[2 * k : 2 * k + 2], (code - 15 * second, second)):
            full = high.astype(jnp.float32)
            values.append(full + digit * (1 / 15) * spacing(full))
    return values


def reduce_kernel(
    rows, chips, chunk, axis,
    len_ref, x_hbm, w_hbm, y_hbm,
    xv, wv, own, give, take, out1, out2, in1, in2, near, fin,
    x_sem, w_sem, give_sem, take_sem, o1_send, o2_send, in1_recv, in2_recv, near_recv,
    fin_send, fin_local, ag_recv, fw_send, fw_recv, sib_send, sib_recv,
    take_free, h1_free, h2_free,
):
    seq_blocks = xv.shape[0] // len_ref.shape[0]
    cols = w_hbm.shape[1]
    half = chunk // 2
    lanes = half // 2
    chunks = cols // chunk
    part = rows // chips
    piece = part // 2
    groups = piece // (2 * ROW_BLOCK)
    me = lax.axis_index(axis)
    chip, core = me // 2, lax.rem(me, 2)
    sib = me + 1 - 2 * core
    right_chip, left_chip, far_chip = lax.rem(chip + 1, chips), lax.rem(chip + chips - 1, chips), lax.rem(chip + 2, chips)
    right, left = right_chip * 2 + core, left_chip * 2 + core

    def at_a(c):
        return c * part

    def at_b(c):
        return c * part + piece

    def rows_from(at, size):
        return pl.ds(pl.multiple_of(at, piece), size)

    def cols_of(j):
        return pl.ds(pl.multiple_of(j * chunk + core * half, half), half)

    def remote(src, dst, send, recv, to):
        return pltpu.make_async_remote_copy(
            src_ref=src, dst_ref=dst, send_sem=send, recv_sem=recv, device_id={axis: to}, device_id_type=MESH
        )

    def signal(sem, to):
        pl.semaphore_signal(sem, inc=1, device_id={axis: to}, device_id_type=MESH)

    def w_copy(j, k):
        s = lax.rem(j, 2)
        side = core if k == 0 else 1 - core
        at = pl.ds(pl.multiple_of(j * chunk + side * half, half), half)
        return pltpu.make_async_copy(w_hbm.at[:, at], wv.at[s, :, pl.ds(k * half, half)], w_sem.at[s, k])

    def give_copy():
        return remote(give, take, give_sem, take_sem, sib)

    def hop1_copy(j, d):
        s, o = lax.rem(j, SLOTS), lax.rem(j, 2)
        return remote(out1.at[o, d], in1.at[s, d], o1_send.at[o, d], in1_recv.at[s, d], (right, left)[d])

    def near_copy(j, d):
        s, o = lax.rem(j, SLOTS), lax.rem(j, 2)
        return remote(out1.at[o, 2 + d], near.at[s, d], o1_send.at[o, 2 + d], near_recv.at[s, d], (left, right)[d])

    def hop2_copy(j, d):
        s, o = lax.rem(j, SLOTS), lax.rem(j, 2)
        return remote(out2.at[o, d], in2.at[s, d], o2_send.at[o, d], in2_recv.at[s, d], (right, left)[d])

    def there(j):
        return y_hbm.at[rows_from(chip * part, part), cols_of(j)]

    def gather_copy(j, d):
        s = lax.rem(j, SLOTS)
        return remote(fin.at[s], there(j), fin_send.at[s, d], ag_recv.at[j, d], (right, left)[d])

    def gather_share(j):
        s = lax.rem(j, SLOTS)
        return remote(fin.at[s], there(j), fin_send.at[s, 2], sib_recv, sib)

    def gather_local(j):
        s = lax.rem(j, SLOTS)
        return pltpu.make_async_copy(fin.at[s], there(j), fin_local.at[s])

    def forward_copy(j, d):
        at = (at_a(left_chip), at_b(right_chip))[d]
        ref = y_hbm.at[rows_from(at, piece), cols_of(j)]
        return remote(ref, ref, fw_send.at[d], fw_recv.at[j, d], (right, left)[d])

    def share_copy(j, c):
        ref = y_hbm.at[rows_from(c * part, part), cols_of(j)]
        return remote(ref, ref, sib_send, sib_recv, sib)

    def wait_gather_sends(j):
        for d in range(2):
            gather_copy(j, d).wait_send()
        gather_share(j).wait_send()
        gather_local(j).wait()

    def wait_first_sends(j):
        for d in range(2):
            hop1_copy(j, d).wait_send()
            near_copy(j, d).wait_send()

    def wait_hop2_sends(j):
        for d in range(2):
            hop2_copy(j, d).wait_send()

    quarters = [(r, c) for r in range(2) for c in range(2)]

    def block_rows(at, r, g):
        return pl.ds(pl.multiple_of(at + r * (piece // 2) + g * ROW_BLOCK, ROW_BLOCK), ROW_BLOCK)

    def block_cols(c):
        return pl.ds(c * lanes, lanes)

    def put(message, g, values):
        highs, word = encode(values)
        for (r, c), high in zip(quarters, highs):
            message[block_rows(c * piece, r, g), :] = high
        message[block_rows(2 * piece, 0, g), :] = word

    def get(message, g):
        highs = [message[block_rows(c * piece, r, g), :] for r, c in quarters]
        return decode(highs, message[block_rows(2 * piece, 0, g), :])

    def blocks_of(ref, at, g):
        return [ref[block_rows(at, r, g), block_cols(c)] for r, c in quarters]

    load_x = pltpu.make_async_copy(x_hbm, xv, x_sem)
    load_x.start()
    for k in range(2):
        w_copy(0, k).start()

    barrier = pltpu.get_barrier_semaphore()
    for to in (left, right, sib):
        signal(barrier, to)
    pl.semaphore_wait(barrier, 3)

    load_x.wait()

    blocks = [(len_ref[k] + ROW_BLOCK - 1) // ROW_BLOCK for k in range(len_ref.shape[0])]
    ends = [sum(blocks[: k + 1]) for k in range(len(blocks))]

    def compact(i, carry):
        src = i
        for k in range(len(blocks)):
            src = src + jnp.where(i >= ends[k], seq_blocks - blocks[k], 0)
        xv[i] = xv[jnp.minimum(src, xv.shape[0] - 1)]
        return carry

    lax.fori_loop(0, rows // ROW_BLOCK, compact, 0)

    def step(t, carry):
        ja, jb, jc, jd, je = t - 1, t - 2, t - 3, t - 4, t - 5

        @pl.when((ja >= 0) & (ja < chunks))
        def _():
            s, o = lax.rem(ja, SLOTS), lax.rem(ja, 2)

            @pl.when(ja >= 2)
            def _():
                wait_first_sends(ja - 2)

            give_copy().wait_recv()

            def body(g, carry):
                for k, at in enumerate((at_a(far_chip), at_b(far_chip), at_a(left_chip), at_b(right_chip))):
                    mine, other = blocks_of(own.at[s], at, g), blocks_of(take, at, g)
                    put(out1.at[o, k], g, [p + q for p, q in zip(mine, other)])
                for at in (at_a(chip), at_b(chip), at_a(right_chip), at_b(left_chip)):
                    for r in range(2):
                        here = block_rows(at, r, g)
                        own[s, here, :] = own[s, here, :] + take[here, :]
                return carry

            lax.fori_loop(0, groups, body, 0)

            @pl.when(ja + 1 < chunks)
            def _():
                signal(take_free, sib)

            @pl.when(ja >= SLOTS)
            def _():
                for d in range(2):
                    pl.semaphore_wait(h1_free.at[d], 1)
                    pl.semaphore_wait(h2_free.at[d], 1)

            for d in range(2):
                hop1_copy(ja, d).start()
            for d in range(2):
                near_copy(ja, d).start()

        @pl.when((jb >= 0) & (jb < chunks))
        def _():
            s, o = lax.rem(jb, SLOTS), lax.rem(jb, 2)

            @pl.when(jb >= 2)
            def _():
                wait_hop2_sends(jb - 2)

            for d in range(2):
                hop1_copy(jb, d).wait_recv()

            def body(g, carry):
                for d, at in enumerate((at_a(right_chip), at_b(left_chip))):
                    mine, other = blocks_of(own.at[s], at, g), get(in1.at[s, d], g)
                    put(out2.at[o, d], g, [p + q for p, q in zip(mine, other)])
                return carry

            lax.fori_loop(0, groups, body, 0)
            for d in range(2):
                hop2_copy(jb, d).start()

            @pl.when(jb + SLOTS < chunks)
            def _():
                signal(h1_free.at[0], left)
                signal(h1_free.at[1], right)

        @pl.when((jc >= 0) & (jc < chunks))
        def _():
            s = lax.rem(jc, SLOTS)
            for d in range(2):
                near_copy(jc, d).wait_recv()
            for d in range(2):
                hop2_copy(jc, d).wait_recv()

            @pl.when(jc >= SLOTS)
            def _():
                wait_gather_sends(jc - SLOTS)

            def body(g, carry):
                for d, at in enumerate((at_a(chip), at_b(chip))):
                    sums = zip(blocks_of(own.at[s], at, g), get(in2.at[s, d], g), get(near.at[s, d], g))
                    for (r, c), (p, q, n) in zip(quarters, sums):
                        fin[s, block_rows(d * piece, r, g), block_cols(c)] = (p + q + n).astype(fin.dtype)
                return carry

            lax.fori_loop(0, groups, body, 0)

            @pl.when(jc + SLOTS < chunks)
            def _():
                signal(h2_free.at[0], left)
                signal(h2_free.at[1], right)

            for d in range(2):
                gather_copy(jc, d).start()
            gather_share(jc).start()
            gather_local(jc).start()

        @pl.when((jd >= 0) & (jd < chunks))
        def _():
            for d, c in enumerate((left_chip, right_chip)):
                gather_copy(jd, d).wait_recv()
                forward_copy(jd, d).start()
                share_copy(jd, c).start()

        @pl.when((je >= 0) & (je < chunks))
        def _():
            for d in range(2):
                forward_copy(je, d).wait_recv()
            share_copy(je, far_chip).start()

        @pl.when(t < chunks)
        def _():
            s, w = lax.rem(t, SLOTS), lax.rem(t, 2)

            @pl.when(t + 1 < chunks)
            def _():
                for k in range(2):
                    w_copy(t + 1, k).start()

            for k in range(2):
                w_copy(t, k).wait()

            @pl.when(t >= 1)
            def _():
                give_copy().wait_send()

            def tile_dot(m, carry):
                x = xv[pl.ds(m * (DOT_ROWS // ROW_BLOCK), DOT_ROWS // ROW_BLOCK)].reshape(DOT_ROWS, xv.shape[2])
                both = jnp.dot(x, wv[w], preferred_element_type=jnp.float32)
                at = pl.ds(pl.multiple_of(m * DOT_ROWS, DOT_ROWS), DOT_ROWS)
                own[s, at, :] = both[:, :half]
                give[at, :] = both[:, half:]
                return carry

            lax.fori_loop(0, rows // DOT_ROWS, tile_dot, 0)

            @pl.when(t >= 1)
            def _():
                pl.semaphore_wait(take_free, 1)

            give_copy().start()

        return carry

    lax.fori_loop(0, chunks + 5, step, 0)

    give_copy().wait_send()
    for k in range(2):
        wait_first_sends(chunks - 2 + k)
        wait_hop2_sends(chunks - 2 + k)
    for k in range(SLOTS):
        wait_gather_sends(chunks - SLOTS + k)
    wide = pl.ds(0, cols // 2)
    for d in range(2):
        ref = y_hbm.at[pl.ds(0, piece), wide]
        remote(ref, ref, fw_send.at[d], sib_recv, sib).wait_send()
    ref = y_hbm.at[pl.ds(0, 3 * part), wide]
    remote(ref, ref, sib_send, sib_recv, sib).wait_send()
    ref = y_hbm.at[pl.ds(0, rows), wide]
    remote(ref, ref, sib_send, sib_recv, sib).wait_recv()


def reduce_rows(rows, y_rows, chips, index, axis, lengths, x, w):
    tokens, inner = x.shape
    cols = w.shape[1]
    half = CHUNK_COLS // 2
    chunks = cols // CHUNK_COLS
    part = rows // chips
    message = (part // 2 * 5 // 2, half // 2)
    dma, regular = pltpu.SemaphoreType.DMA, pltpu.SemaphoreType.REGULAR
    f32, bf16 = jnp.float32, jnp.bfloat16
    any_spec = pl.BlockSpec(memory_space=pl.ANY)
    return pl.pallas_call(
        functools.partial(reduce_kernel, rows, chips, CHUNK_COLS, axis),
        out_shape=jax.ShapeDtypeStruct((y_rows, cols), bf16),
        in_specs=[pl.BlockSpec(memory_space=pltpu.SMEM), any_spec, any_spec],
        out_specs=any_spec,
        scratch_shapes=[
            pltpu.VMEM((tokens // ROW_BLOCK, ROW_BLOCK, inner), x.dtype),
            pltpu.VMEM((2, inner, CHUNK_COLS), w.dtype),
            pltpu.VMEM((SLOTS, rows, half), f32),
            pltpu.VMEM((rows, half), f32),
            pltpu.VMEM((rows, half), f32),
            pltpu.VMEM((2, 4, *message), bf16),
            pltpu.VMEM((2, 2, *message), bf16),
            pltpu.VMEM((SLOTS, 2, *message), bf16),
            pltpu.VMEM((SLOTS, 2, *message), bf16),
            pltpu.VMEM((SLOTS, 2, *message), bf16),
            pltpu.VMEM((SLOTS, part, half), bf16),
            dma, dma((2, 2)), dma, dma,
            dma((2, 4)), dma((2, 2)), dma((SLOTS, 2)), dma((SLOTS, 2)), dma((SLOTS, 2)),
            dma((SLOTS, 3)), dma((SLOTS,)), dma((chunks, 2)), dma((2,)), dma((chunks, 2)), dma, dma,
            regular, regular((2,)), regular((2,)),
        ],
        compiler_params=pltpu.CompilerParams(
            collective_id=index, has_side_effects=True, vmem_limit_bytes=67043328
        ),
        cost_estimate=pl.CostEstimate(
            flops=2 * rows * inner * cols, bytes_accessed=2 * (tokens * inner + inner * cols + rows * cols), transcendentals=0
        ),
        name=f"reduce_{rows}",
    )(lengths, x.reshape(tokens // ROW_BLOCK, ROW_BLOCK, inner), w)


def bucket_kernel(sizes, peers, axis, len_ref, out_ref, mine, theirs, send_sem, recv_sem):
    me = lax.axis_index(axis)
    rows = sum((len_ref[k] + ROW_BLOCK - 1) // ROW_BLOCK for k in range(len_ref.shape[0])) * ROW_BLOCK
    bucket = sum((rows > size).astype(jnp.int32) for size in sizes[:-1])
    mine[...] = jnp.full(mine.shape, bucket, jnp.int32).astype(jnp.float32)
    others = [lax.rem(me + k, peers) for k in range(1, peers)]
    barrier = pltpu.get_barrier_semaphore()
    for to in others:
        pl.semaphore_signal(barrier, inc=1, device_id={axis: to}, device_id_type=MESH)
    pl.semaphore_wait(barrier, peers - 1)
    copies = [
        pltpu.make_async_remote_copy(
            src_ref=mine, dst_ref=theirs.at[k], send_sem=send_sem.at[k], recv_sem=recv_sem.at[k],
            device_id={axis: to}, device_id_type=MESH,
        )
        for k, to in enumerate(others)
    ]
    for c in copies:
        c.start()
    most = mine[...]
    for k, c in enumerate(copies):
        c.wait()
        most = jnp.maximum(most, theirs[k])
    out_ref[0] = jnp.max(most).astype(jnp.int32)


def pick_bucket(sizes, peers, index, axis, lengths):
    return pl.pallas_call(
        functools.partial(bucket_kernel, sizes, peers, axis),
        out_shape=jax.ShapeDtypeStruct((1,), jnp.int32),
        in_specs=[pl.BlockSpec(memory_space=pltpu.SMEM)],
        out_specs=pl.BlockSpec(memory_space=pltpu.SMEM),
        scratch_shapes=[
            pltpu.VMEM((8, 128), jnp.float32),
            pltpu.VMEM((peers - 1, 8, 128), jnp.float32),
            pltpu.SemaphoreType.DMA((peers - 1,)),
            pltpu.SemaphoreType.DMA((peers - 1,)),
        ],
        compiler_params=pltpu.CompilerParams(collective_id=index, has_side_effects=True),
        name="bucket",
    )(lengths)[0]


def tile_source(i, len_ref, tiles):
    slot, offset = i // tiles, lax.rem(i, tiles) * OUT_TILE
    first, length = 0, 0
    for k in range(len_ref.shape[0]):
        first = first + jnp.where(k < slot, (len_ref[k] + ROW_BLOCK - 1) // ROW_BLOCK, 0)
        length = length + jnp.where(k == slot, len_ref[k], 0)
    last = (length - 1) // OUT_TILE * OUT_TILE
    return offset, length, first + jnp.minimum(offset, last) // ROW_BLOCK


def expand_kernel(tiles, len_ref, y_ref, out_ref):
    offset, length, _ = tile_source(pl.program_id(0), len_ref, tiles)
    row = lax.broadcasted_iota(jnp.int32, (out_ref.shape[0], 1), 0)
    y = y_ref[...]
    out_ref[...] = jnp.where(row < length - offset, y, jnp.zeros_like(y))


def expand_rows(tokens, lengths, y):
    cols = y.shape[1]
    tiles = tokens // lengths.shape[0] // OUT_TILE
    return pl.pallas_call(
        functools.partial(expand_kernel, tiles),
        out_shape=jax.ShapeDtypeStruct((tokens, cols), y.dtype),
        grid_spec=pltpu.PrefetchScalarGridSpec(
            num_scalar_prefetch=1,
            grid=(tokens // OUT_TILE,),
            in_specs=[
                pl.BlockSpec(
                    (pl.Element(OUT_TILE), pl.Element(cols)),
                    lambda i, len_ref: (tile_source(i, len_ref, tiles)[2] * ROW_BLOCK, 0),
                )
            ],
            out_specs=pl.BlockSpec((OUT_TILE, cols), lambda i, len_ref: (i, 0)),
        ),
        compiler_params=pltpu.CompilerParams(vmem_limit_bytes=48 * 2**20),
        name="expand",
    )(lengths, y)


def solution(mesh):
    chips = mesh.shape["tp"] // 2

    def local_part(x_loc, w_loc, lengths):
        tokens = x_loc.shape[0]
        slots = lengths.shape[0]
        seq_len = tokens // slots
        most = (slots - 1) * seq_len + ROW_BLOCK
        least = seq_len + (slots - 1) * ROW_BLOCK
        sizes = [-(-least // BUCKET_STEP) * BUCKET_STEP]
        while sizes[-1] < most:
            sizes.append(sizes[-1] + BUCKET_STEP)
        y_rows = sizes[-1] + OUT_TILE
        bucket = pick_bucket(sizes, mesh.shape["data"], len(sizes), "data", lengths)
        branches = [
            functools.partial(reduce_rows, rows, y_rows, chips, k, "tp") for k, rows in enumerate(sizes)
        ]
        y = lax.switch(bucket, branches, lengths, x_loc, w_loc)
        return expand_rows(tokens, lengths, y)

    return jax.shard_map(
        local_part,
        mesh=mesh,
        in_specs=(P("data", "tp"), P("tp", None), P("data")),
        out_specs=P("data", None),
        check_vma=False,
    )
```

```python
import functools

import jax
import jax.numpy as jnp
from jax import lax
from jax.experimental import pallas as pl
from jax.experimental.pallas import tpu as pltpu
from jax.sharding import PartitionSpec as P

MESH = pl.DeviceIdType.MESH
ROW_BLOCK = 16
BUCKET_STEP = 128
CHUNK_COLS = 512
OUT_TILE = 256
SLOTS = 3
DOT_ROWS = 256
BF16_MAX = float(jnp.finfo(jnp.bfloat16).max)


def spacing(high):
    size = jnp.abs(high)
    above = (size * (1 + 0.75 / 128)).astype(jnp.bfloat16).astype(jnp.float32)
    return jnp.clip(above - size, 2.0**-120, 2.0**120)


def encode(values):
    highs, digits = [], []
    for v in values:
        high = jnp.clip(v, -BF16_MAX, BF16_MAX).astype(jnp.bfloat16)
        full = high.astype(jnp.float32)
        rest = (v - full) / spacing(full)
        highs.append(high)
        digits.append(jnp.clip(jnp.floor(rest * 15 + 0.5), -7, 7))
    n = digits[0] + 15 * digits[1] + 112
    e = digits[2] + 15 * digits[3]
    word = jnp.where(n < 128, n + 128, -n) * jnp.exp2(e)
    return highs, word.astype(jnp.bfloat16)


def decode(highs, word):
    word = word.astype(jnp.float32)
    size = jnp.abs(word)
    e = jnp.floor(jnp.log2(size) + (0.002 - 7))
    m = jnp.floor(size * jnp.exp2(-e) + 0.5)
    n = jnp.where(word > 0, m - 240, m - 112)
    values = []
    for k, code in enumerate((n, e)):
        second = jnp.floor(code * (1 / 15) + 0.5)
        for high, digit in zip(highs[2 * k : 2 * k + 2], (code - 15 * second, second)):
            full = high.astype(jnp.float32)
            values.append(full + digit * (1 / 15) * spacing(full))
    return values


def reduce_kernel(
    rows, chips, chunk, axis,
    len_ref, x_hbm, w_hbm, y_hbm,
    xv, wv, own, give, take, out1, out2, in1, in2, near, fin,
    x_sem, w_sem, give_sem, take_sem, o1_send, o2_send, in1_recv, in2_recv, near_recv,
    fin_send, fin_local, ag_recv, fw_send, fw_recv, sib_send, sib_recv,
    take_free, h1_free, h2_free,
):
    seq_blocks = xv.shape[0] // len_ref.shape[0]
    cols = w_hbm.shape[1]
    half = chunk // 2
    lanes = half // 2
    chunks = cols // chunk
    part = rows // chips
    piece = part // 2
    groups = -(-piece // (2 * ROW_BLOCK))
    tiles = -(-rows // DOT_ROWS)
    me = lax.axis_index(axis)
    chip, core = me // 2, lax.rem(me, 2)
    sib = me + 1 - 2 * core
    right_chip, left_chip, far_chip = lax.rem(chip + 1, chips), lax.rem(chip + chips - 1, chips), lax.rem(chip + 2, chips)
    right, left = right_chip * 2 + core, left_chip * 2 + core

    def at_a(c):
        return c * part

    def at_b(c):
        return c * part + piece

    def rows_from(at, size):
        return pl.ds(pl.multiple_of(at, piece), size)

    def cols_of(j):
        return pl.ds(pl.multiple_of(j * chunk + core * half, half), half)

    def remote(src, dst, send, recv, to):
        return pltpu.make_async_remote_copy(
            src_ref=src, dst_ref=dst, send_sem=send, recv_sem=recv, device_id={axis: to}, device_id_type=MESH
        )

    def signal(sem, to):
        pl.semaphore_signal(sem, inc=1, device_id={axis: to}, device_id_type=MESH)

    def w_copy(j, k):
        s = lax.rem(j, 2)
        side = core if k == 0 else 1 - core
        at = pl.ds(pl.multiple_of(j * chunk + side * half, half), half)
        return pltpu.make_async_copy(w_hbm.at[:, at], wv.at[s, :, pl.ds(k * half, half)], w_sem.at[s, k])

    def give_copy():
        return remote(give, take, give_sem, take_sem, sib)

    def hop1_copy(j, d):
        s, o = lax.rem(j, SLOTS), lax.rem(j, 2)
        return remote(out1.at[o, d], in1.at[s, d], o1_send.at[o, d], in1_recv.at[s, d], (right, left)[d])

    def near_copy(j, d):
        s, o = lax.rem(j, SLOTS), lax.rem(j, 2)
        return remote(out1.at[o, 2 + d], near.at[s, d], o1_send.at[o, 2 + d], near_recv.at[s, d], (left, right)[d])

    def hop2_copy(j, d):
        s, o = lax.rem(j, SLOTS), lax.rem(j, 2)
        return remote(out2.at[o, d], in2.at[s, d], o2_send.at[o, d], in2_recv.at[s, d], (right, left)[d])

    def there(j):
        return y_hbm.at[rows_from(chip * part, part), cols_of(j)]

    def gather_copy(j, d):
        s = lax.rem(j, SLOTS)
        return remote(fin.at[s], there(j), fin_send.at[s, d], ag_recv.at[j, d], (right, left)[d])

    def gather_share(j):
        s = lax.rem(j, SLOTS)
        return remote(fin.at[s], there(j), fin_send.at[s, 2], sib_recv, sib)

    def gather_local(j):
        s = lax.rem(j, SLOTS)
        return pltpu.make_async_copy(fin.at[s], there(j), fin_local.at[s])

    def forward_copy(j, d):
        at = (at_a(left_chip), at_b(right_chip))[d]
        ref = y_hbm.at[rows_from(at, piece), cols_of(j)]
        return remote(ref, ref, fw_send.at[d], fw_recv.at[j, d], (right, left)[d])

    def share_copy(j, c):
        ref = y_hbm.at[rows_from(c * part, part), cols_of(j)]
        return remote(ref, ref, sib_send, sib_recv, sib)

    def wait_gather_sends(j):
        for d in range(2):
            gather_copy(j, d).wait_send()
        gather_share(j).wait_send()
        gather_local(j).wait()

    def wait_first_sends(j):
        for d in range(2):
            hop1_copy(j, d).wait_send()
            near_copy(j, d).wait_send()

    def wait_hop2_sends(j):
        for d in range(2):
            hop2_copy(j, d).wait_send()

    quarters = [(r, c) for r in range(2) for c in range(2)]

    def block_rows(at, r, g):
        first = jnp.minimum(g * 2 * ROW_BLOCK, piece - 2 * ROW_BLOCK)
        return pl.ds(pl.multiple_of(at + first + r * ROW_BLOCK, ROW_BLOCK), ROW_BLOCK)

    def word_rows(g):
        return pl.ds(pl.multiple_of(2 * piece + g * ROW_BLOCK, ROW_BLOCK), ROW_BLOCK)

    def block_cols(c):
        return pl.ds(c * lanes, lanes)

    def put(message, g, values):
        highs, word = encode(values)
        for (r, c), high in zip(quarters, highs):
            message[block_rows(c * piece, r, g), :] = high
        message[word_rows(g), :] = word

    def get(message, g):
        highs = [message[block_rows(c * piece, r, g), :] for r, c in quarters]
        return decode(highs, message[word_rows(g), :])

    def blocks_of(ref, at, g):
        return [ref[block_rows(at, r, g), block_cols(c)] for r, c in quarters]

    load_x = pltpu.make_async_copy(x_hbm, xv, x_sem)
    load_x.start()
    for k in range(2):
        w_copy(0, k).start()

    barrier = pltpu.get_barrier_semaphore()
    for to in (left, right, sib):
        signal(barrier, to)

    blocks = [(len_ref[k] + ROW_BLOCK - 1) // ROW_BLOCK for k in range(len_ref.shape[0])]
    ends = [sum(blocks[: k + 1]) for k in range(len(blocks))]

    def compact(i, carry):
        src = i
        for k in range(len(blocks)):
            src = src + jnp.where(i >= ends[k], seq_blocks - blocks[k], 0)
        xv[i] = xv[jnp.minimum(src, xv.shape[0] - 1)]
        return carry

    load_x.wait()
    lax.fori_loop(0, rows // ROW_BLOCK, compact, 0)
    pl.semaphore_wait(barrier, 3)

    def tile_rows(m):
        return pl.ds(pl.multiple_of(jnp.minimum(m * DOT_ROWS, rows - DOT_ROWS), ROW_BLOCK), DOT_ROWS)

    def tile_x(m):
        at = jnp.minimum(m * (DOT_ROWS // ROW_BLOCK), (rows - DOT_ROWS) // ROW_BLOCK)
        return xv[pl.ds(at, DOT_ROWS // ROW_BLOCK)].reshape(DOT_ROWS, xv.shape[2])

    def step(t, carry):
        ja, jb, jc, jd, je = t - 1, t - 2, t - 3, t - 4, t - 5

        @pl.when((ja >= 0) & (ja < chunks))
        def _():
            s, o = lax.rem(ja, SLOTS), lax.rem(ja, 2)

            @pl.when(ja >= 2)
            def _():
                wait_first_sends(ja - 2)

            give_copy().wait_recv()

            def body(g, carry):
                for k, at in enumerate((at_a(far_chip), at_b(far_chip), at_a(left_chip), at_b(right_chip))):
                    mine, other = blocks_of(own.at[s], at, g), blocks_of(take, at, g)
                    put(out1.at[o, k], g, [p + q for p, q in zip(mine, other)])
                return carry

            lax.fori_loop(0, groups, body, 0)

            @pl.when(ja >= SLOTS)
            def _():
                for d in range(2):
                    pl.semaphore_wait(h1_free.at[d], 1)
                    pl.semaphore_wait(h2_free.at[d], 1)

            for d in range(2):
                hop1_copy(ja, d).start()
            for d in range(2):
                near_copy(ja, d).start()

            def keep(i, carry):
                for at in (at_a(chip), at_b(chip), at_a(right_chip), at_b(left_chip)):
                    here = pl.ds(pl.multiple_of(at + i * ROW_BLOCK, ROW_BLOCK), ROW_BLOCK)
                    own[s, here, :] = own[s, here, :] + take[here, :]
                return carry

            lax.fori_loop(0, piece // ROW_BLOCK, keep, 0)

            @pl.when(ja + 1 < chunks)
            def _():
                signal(take_free, sib)

        @pl.when((jb >= 0) & (jb < chunks))
        def _():
            s, o = lax.rem(jb, SLOTS), lax.rem(jb, 2)

            @pl.when(jb >= 2)
            def _():
                wait_hop2_sends(jb - 2)

            for d in range(2):
                hop1_copy(jb, d).wait_recv()

            def body(g, carry):
                for d, at in enumerate((at_a(right_chip), at_b(left_chip))):
                    mine, other = blocks_of(own.at[s], at, g), get(in1.at[s, d], g)
                    put(out2.at[o, d], g, [p + q for p, q in zip(mine, other)])
                return carry

            lax.fori_loop(0, groups, body, 0)
            for d in range(2):
                hop2_copy(jb, d).start()

            @pl.when(jb + SLOTS < chunks)
            def _():
                signal(h1_free.at[0], left)
                signal(h1_free.at[1], right)

        @pl.when((jc >= 0) & (jc < chunks))
        def _():
            s = lax.rem(jc, SLOTS)
            for d in range(2):
                near_copy(jc, d).wait_recv()
            for d in range(2):
                hop2_copy(jc, d).wait_recv()

            @pl.when(jc >= SLOTS)
            def _():
                wait_gather_sends(jc - SLOTS)

            def body(g, carry):
                for d, at in enumerate((at_a(chip), at_b(chip))):
                    sums = zip(blocks_of(own.at[s], at, g), get(in2.at[s, d], g), get(near.at[s, d], g))
                    for (r, c), (p, q, n) in zip(quarters, sums):
                        fin[s, block_rows(d * piece, r, g), block_cols(c)] = (p + q + n).astype(fin.dtype)
                return carry

            lax.fori_loop(0, groups, body, 0)

            @pl.when(jc + SLOTS < chunks)
            def _():
                signal(h2_free.at[0], left)
                signal(h2_free.at[1], right)

            for d in range(2):
                gather_copy(jc, d).start()
            gather_share(jc).start()
            gather_local(jc).start()

        @pl.when((jd >= 0) & (jd < chunks))
        def _():
            for d, c in enumerate((left_chip, right_chip)):
                gather_copy(jd, d).wait_recv()
                forward_copy(jd, d).start()
                share_copy(jd, c).start()

        @pl.when((je >= 0) & (je < chunks))
        def _():
            for d in range(2):
                forward_copy(je, d).wait_recv()
            share_copy(je, far_chip).start()

        @pl.when(t < chunks)
        def _():
            s, w = lax.rem(t, SLOTS), lax.rem(t, 2)

            @pl.when(t + 1 < chunks)
            def _():
                for k in range(2):
                    w_copy(t + 1, k).start()

            for k in range(2):
                w_copy(t, k).wait()

            @pl.when(t >= 1)
            def _():
                give_copy().wait_send()

            def give_dot(m, carry):
                give[tile_rows(m), :] = jnp.dot(tile_x(m), wv[w, :, half:], preferred_element_type=jnp.float32)
                return carry

            def own_dot(m, carry):
                own[s, tile_rows(m), :] = jnp.dot(tile_x(m), wv[w, :, :half], preferred_element_type=jnp.float32)
                return carry

            lax.fori_loop(0, tiles, give_dot, 0)
            @pl.when(t >= 1)
            def _():
                pl.semaphore_wait(take_free, 1)

            give_copy().start()
            lax.fori_loop(0, tiles, own_dot, 0)

        return carry

    lax.fori_loop(0, chunks + 5, step, 0)

    give_copy().wait_send()
    for k in range(2):
        wait_first_sends(chunks - 2 + k)
        wait_hop2_sends(chunks - 2 + k)
    for k in range(SLOTS):
        wait_gather_sends(chunks - SLOTS + k)
    wide = pl.ds(0, cols // 2)
    for d in range(2):
        ref = y_hbm.at[pl.ds(0, piece), wide]
        remote(ref, ref, fw_send.at[d], sib_recv, sib).wait_send()
    ref = y_hbm.at[pl.ds(0, 3 * part), wide]
    remote(ref, ref, sib_send, sib_recv, sib).wait_send()
    ref = y_hbm.at[pl.ds(0, rows), wide]
    remote(ref, ref, sib_send, sib_recv, sib).wait_recv()


def reduce_rows(rows, y_rows, chips, index, axis, lengths, x, w):
    tokens, inner = x.shape
    cols = w.shape[1]
    half = CHUNK_COLS // 2
    chunks = cols // CHUNK_COLS
    part = rows // chips
    piece = part // 2
    message = (2 * piece + -(-piece // (2 * ROW_BLOCK)) * ROW_BLOCK, half // 2)
    dma, regular = pltpu.SemaphoreType.DMA, pltpu.SemaphoreType.REGULAR
    f32, bf16 = jnp.float32, jnp.bfloat16
    any_spec = pl.BlockSpec(memory_space=pl.ANY)
    return pl.pallas_call(
        functools.partial(reduce_kernel, rows, chips, CHUNK_COLS, axis),
        out_shape=jax.ShapeDtypeStruct((y_rows, cols), bf16),
        in_specs=[pl.BlockSpec(memory_space=pltpu.SMEM), any_spec, any_spec],
        out_specs=any_spec,
        scratch_shapes=[
            pltpu.VMEM((tokens // ROW_BLOCK, ROW_BLOCK, inner), x.dtype),
            pltpu.VMEM((2, inner, CHUNK_COLS), w.dtype),
            pltpu.VMEM((SLOTS, rows, half), f32),
            pltpu.VMEM((rows, half), f32),
            pltpu.VMEM((rows, half), f32),
            pltpu.VMEM((2, 4, *message), bf16),
            pltpu.VMEM((2, 2, *message), bf16),
            pltpu.VMEM((SLOTS, 2, *message), bf16),
            pltpu.VMEM((SLOTS, 2, *message), bf16),
            pltpu.VMEM((SLOTS, 2, *message), bf16),
            pltpu.VMEM((SLOTS, part, half), bf16),
            dma, dma((2, 2)), dma, dma,
            dma((2, 4)), dma((2, 2)), dma((SLOTS, 2)), dma((SLOTS, 2)), dma((SLOTS, 2)),
            dma((SLOTS, 3)), dma((SLOTS,)), dma((chunks, 2)), dma((2,)), dma((chunks, 2)), dma, dma,
            regular, regular((2,)), regular((2,)),
        ],
        compiler_params=pltpu.CompilerParams(
            collective_id=index, has_side_effects=True, vmem_limit_bytes=67043328
        ),
        cost_estimate=pl.CostEstimate(
            flops=2 * rows * inner * cols, bytes_accessed=2 * (tokens * inner + inner * cols + rows * cols), transcendentals=0
        ),
        name=f"reduce_{rows}",
    )(lengths, x.reshape(tokens // ROW_BLOCK, ROW_BLOCK, inner), w)


def bucket_kernel(sizes, peers, axis, len_ref, out_ref, mine, theirs, send_sem, recv_sem):
    me = lax.axis_index(axis)
    rows = sum((len_ref[k] + ROW_BLOCK - 1) // ROW_BLOCK for k in range(len_ref.shape[0])) * ROW_BLOCK
    bucket = sum((rows > size).astype(jnp.int32) for size in sizes[:-1])
    mine[...] = jnp.full(mine.shape, bucket, jnp.int32).astype(jnp.float32)
    others = [lax.rem(me + k, peers) for k in range(1, peers)]
    barrier = pltpu.get_barrier_semaphore()
    for to in others:
        pl.semaphore_signal(barrier, inc=1, device_id={axis: to}, device_id_type=MESH)
    pl.semaphore_wait(barrier, peers - 1)
    copies = [
        pltpu.make_async_remote_copy(
            src_ref=mine, dst_ref=theirs.at[k], send_sem=send_sem.at[k], recv_sem=recv_sem.at[k],
            device_id={axis: to}, device_id_type=MESH,
        )
        for k, to in enumerate(others)
    ]
    for c in copies:
        c.start()
    most = mine[...]
    for k, c in enumerate(copies):
        c.wait()
        most = jnp.maximum(most, theirs[k])
    out_ref[0] = jnp.max(most).astype(jnp.int32)


def pick_bucket(sizes, peers, index, axis, lengths):
    return pl.pallas_call(
        functools.partial(bucket_kernel, sizes, peers, axis),
        out_shape=jax.ShapeDtypeStruct((1,), jnp.int32),
        in_specs=[pl.BlockSpec(memory_space=pltpu.SMEM)],
        out_specs=pl.BlockSpec(memory_space=pltpu.SMEM),
        scratch_shapes=[
            pltpu.VMEM((8, 128), jnp.float32),
            pltpu.VMEM((peers - 1, 8, 128), jnp.float32),
            pltpu.SemaphoreType.DMA((peers - 1,)),
            pltpu.SemaphoreType.DMA((peers - 1,)),
        ],
        compiler_params=pltpu.CompilerParams(collective_id=index, has_side_effects=True),
        name="bucket",
    )(lengths)[0]


def tile_source(i, len_ref, tiles):
    slot, offset = i // tiles, lax.rem(i, tiles) * OUT_TILE
    first, length = 0, 0
    for k in range(len_ref.shape[0]):
        first = first + jnp.where(k < slot, (len_ref[k] + ROW_BLOCK - 1) // ROW_BLOCK, 0)
        length = length + jnp.where(k == slot, len_ref[k], 0)
    last = (length - 1) // OUT_TILE * OUT_TILE
    return offset, length, first + jnp.minimum(offset, last) // ROW_BLOCK


def expand_kernel(tiles, len_ref, y_ref, out_ref):
    offset, length, _ = tile_source(pl.program_id(0), len_ref, tiles)
    row = lax.broadcasted_iota(jnp.int32, (out_ref.shape[0], 1), 0)
    y = y_ref[...]
    out_ref[...] = jnp.where(row < length - offset, y, jnp.zeros_like(y))


def expand_rows(tokens, lengths, y):
    cols = y.shape[1]
    tiles = tokens // lengths.shape[0] // OUT_TILE
    return pl.pallas_call(
        functools.partial(expand_kernel, tiles),
        out_shape=jax.ShapeDtypeStruct((tokens, cols), y.dtype),
        grid_spec=pltpu.PrefetchScalarGridSpec(
            num_scalar_prefetch=1,
            grid=(tokens // OUT_TILE,),
            in_specs=[
                pl.BlockSpec(
                    (pl.Element(OUT_TILE), pl.Element(cols)),
                    lambda i, len_ref: (tile_source(i, len_ref, tiles)[2] * ROW_BLOCK, 0),
                )
            ],
            out_specs=pl.BlockSpec((OUT_TILE, cols), lambda i, len_ref: (i, 0)),
        ),
        compiler_params=pltpu.CompilerParams(vmem_limit_bytes=48 * 2**20),
        name="expand",
    )(lengths, y)


def solution(mesh):
    chips = mesh.shape["tp"] // 2

    def local_part(x_loc, w_loc, lengths):
        tokens = x_loc.shape[0]
        slots = lengths.shape[0]
        seq_len = tokens // slots
        most = (slots - 1) * seq_len + ROW_BLOCK
        least = seq_len + (slots - 1) * ROW_BLOCK
        sizes = [-(-least // (2 * BUCKET_STEP)) * 2 * BUCKET_STEP]
        while sizes[-1] < most:
            sizes.append(sizes[-1] + BUCKET_STEP * (2 if sizes[-1] < tokens * 7 // 16 else 1))
        y_rows = sizes[-1] + OUT_TILE
        bucket = pick_bucket(sizes, mesh.shape["data"], len(sizes), "data", lengths)
        branches = [
            functools.partial(reduce_rows, rows, y_rows, chips, k, "tp") for k, rows in enumerate(sizes)
        ]
        y = lax.switch(bucket, branches, lengths, x_loc, w_loc)
        return expand_rows(tokens, lengths, y)

    return jax.shard_map(
        local_part,
        mesh=mesh,
        in_specs=(P("data", "tp"), P("tp", None), P("data")),
        out_specs=P("data", None),
        check_vma=False,
    )
```
